32 devices in a mesh: scan: 16 (over z, x, core), tile: 2 (over y).
Axes of the slice: x: 2, y: 2, z: 4, core: 2. Of those that a mesh axis runs over, the one named last changes fastest.
Arguments:
- probe_modes: float32 [12, 2, 128, 128], replicated, may hold values from -5 to 5
- patterns: float32 [128, 128, 128], P(('scan', 'tile')), may hold values from 0.005 to 300
- specimen: float32 [2, 2048, 512], P(None, 'scan', 'tile'), may hold values from -17.5 to 17.5
- offsets: int32 [128, 2], P(('scan', 'tile')), may hold values from -128 to 2048, as said below
Outputs:
- new_probe: float32 [12, 2, 128, 128], replicated
- new_specimen: float32 [2, 2048, 512], P(None, 'scan', 'tile')
The draws below stay inside these ranges and needn't reach their ends.
Inputs may be any that keep to these rules, and one draw needn't show every extreme that they name: `offsets`: position p lies in aligned block b = p // 4, held by the device of scan index s = b // (the number of tile devices) and tile index t = b % (the number of tile devices); its row offset lies in s * 128 - 128 to s * 128 + 128, its column offset in t * 256 - 128 to t * 256 + 256, both ends included; in every block one position has its row offset at the lower end and its column offset at the upper end, and one has its row offset at the upper end.
All inputs are finite; a program needn't handle non-finite values.
Results may differ from the reference program's by a relative error of at most 0.0001.
Values sent between devices are 32-bit elements; how exact they have to be, the bound alone decides.
A program may use at most 64 MiB of HBM per device.

```python
import math
import jax
import jax.numpy as jnp
from jax import lax

DET = 128
MODES = 12
P_DEV = 4
ROWS_DEV = 128
COLS_DEV = 256
NS_STEPS = 8
POSITIONS = 128
OBJ_ROWS = 2048
OBJ_COLS = 512


def draw_probe_modes(key, part):
    key_base, key_weight = jax.random.split(key, 2)
    shape_all = (MODES, 2, DET, DET)
    base_field = jnp.clip(jax.random.normal(key_base, shape_all, jnp.float32), -5.0, 5.0)
    weights = jnp.exp(jax.random.uniform(key_weight, (MODES,), jnp.float32, math.log(0.1), math.log(0.4)))
    mixing = 0.6
    weights = weights.at[0].set(1.0)
    mixed = base_field + mixing * base_field[0:1]
    mixed = mixed.at[0].set(base_field[0])
    return (mixed * weights[:, None, None, None]).astype(jnp.float32)


def draw_patterns(key, part):
    key_flux, key_pixel, key_speckle = jax.random.split(key, 3)
    block_count = POSITIONS // P_DEV
    along = (jnp.arange(POSITIONS, dtype=jnp.int32) // P_DEV).astype(jnp.float32) / max(block_count - 1, 1)
    flux_low, flux_high, growth, speck_low, speck_high = (1.0, 6.0, 3.0, 0.2, 1.8)
    flux = jnp.exp(jax.random.uniform(key_flux, (POSITIONS,), jnp.float32, math.log(flux_low), math.log(flux_high))) * growth ** along
    pixel_gain = jnp.exp(jax.random.uniform(key_pixel, (DET, DET), jnp.float32, math.log(0.3), math.log(3.0)))
    speckle = jax.random.uniform(key_speckle, (POSITIONS, DET, DET), jnp.float32, speck_low, speck_high)
    return (flux[:, None, None] * pixel_gain[None] * speckle).astype(jnp.float32)


def draw_specimen(key, part):
    key_values, key_rows, key_cols = jax.random.split(key, 3)
    values = 0.4 * jnp.clip(jax.random.normal(key_values, (2, OBJ_ROWS, OBJ_COLS), jnp.float32), -4.0, 4.0)
    mean_part = 1.0
    row_scale = jnp.exp(jax.random.uniform(key_rows, (OBJ_ROWS,), jnp.float32, math.log(0.5), math.log(2.0)))
    col_scale = jnp.exp(jax.random.uniform(key_cols, (OBJ_COLS,), jnp.float32, math.log(0.5), math.log(2.0)))
    rough = values * row_scale[None, :, None] * col_scale[None, None, :]
    shift = jnp.array([mean_part, 0.0], jnp.float32)[:, None, None]
    return (rough + shift).astype(jnp.float32)


def draw_offsets(key, part):
    key_rows, key_cols = jax.random.split(key, 2)
    tile_count = OBJ_COLS // COLS_DEV
    position = jnp.arange(POSITIONS, dtype=jnp.int32)
    group_index = position // P_DEV
    within = position % P_DEV
    scan_index = group_index // tile_count
    tile_index = group_index % tile_count
    local_row = jax.random.randint(key_rows, (POSITIONS,), 0, ROWS_DEV + DET + 1, dtype=jnp.int32)
    local_col = jax.random.randint(key_cols, (POSITIONS,), 0, COLS_DEV + DET + 1, dtype=jnp.int32)
    local_row = jnp.where(within == 0, 0, jnp.where(within == 1, ROWS_DEV + DET, local_row))
    local_col = jnp.where(within == 0, COLS_DEV + DET, local_col)
    row_offsets = scan_index * ROWS_DEV - DET + local_row
    col_offsets = tile_index * COLS_DEV - DET + local_col
    return jnp.stack([row_offsets, col_offsets], axis=1).astype(jnp.int32)


def setup_inputs(seed: int = 0) -> dict:
    splits = jax.random.split(jax.random.key(seed), 5)
    return {
        "probe_modes": draw_probe_modes(jax.random.fold_in(splits[4], 71), 0),
        "patterns": draw_patterns(jax.random.fold_in(splits[4], 71), 0),
        "specimen": draw_specimen(jax.random.fold_in(splits[4], 71), 0),
        "offsets": draw_offsets(jax.random.fold_in(splits[4], 71), 0),
    }


highest = lax.Precision.HIGHEST
light_floor = 0.05
object_reg = 0.5
probe_reg = 1.0
total_eps = 1e-06

def newton_steps(gram_re, gram_im):
    mode_count = gram_re.shape[0]
    upper = jnp.concatenate([gram_re, -gram_im], axis=1)
    lower = jnp.concatenate([gram_im, gram_re], axis=1)
    embedded = jnp.concatenate([upper, lower], axis=0)
    frobenius = jnp.sqrt(jnp.sum(embedded * embedded))
    identity = jnp.eye(2 * mode_count, dtype=jnp.float32)
    current = embedded / frobenius
    inverse = identity
    for repeat in range(NS_STEPS):
        factor = 1.5 * identity - 0.5 * jnp.dot(inverse, current, precision=highest, preferred_element_type=jnp.float32)
        current = jnp.dot(current, factor, precision=highest, preferred_element_type=jnp.float32)
        inverse = jnp.dot(factor, inverse, precision=highest, preferred_element_type=jnp.float32)
    inverse = inverse / jnp.sqrt(frobenius)
    return (inverse[:mode_count, :mode_count], inverse[mode_count:, :mode_count])

def gram_parts(mode_rows):
    real_rows = mode_rows[0::2]
    imag_rows = mode_rows[1::2]
    gram_re = jnp.dot(real_rows, real_rows.T, precision=highest, preferred_element_type=jnp.float32) + jnp.dot(imag_rows, imag_rows.T, precision=highest, preferred_element_type=jnp.float32)
    gram_im = jnp.dot(real_rows, imag_rows.T, precision=highest, preferred_element_type=jnp.float32) - jnp.dot(imag_rows, real_rows.T, precision=highest, preferred_element_type=jnp.float32)
    return (gram_re, gram_im)

def orthonormal_rows(mode_rows, gram_re, gram_im, power_ratio):
    real_rows = mode_rows[0::2]
    imag_rows = mode_rows[1::2]
    mix_re, mix_im = newton_steps(gram_re, gram_im)
    ortho_re = jnp.dot(mix_re.T, real_rows, precision=highest, preferred_element_type=jnp.float32) - jnp.dot(mix_im.T, imag_rows, precision=highest, preferred_element_type=jnp.float32)
    ortho_im = jnp.dot(mix_im.T, real_rows, precision=highest, preferred_element_type=jnp.float32) + jnp.dot(mix_re.T, imag_rows, precision=highest, preferred_element_type=jnp.float32)
    weight = jnp.sqrt(power_ratio * jnp.diagonal(gram_re))
    joined = jnp.stack([ortho_re, ortho_im], axis=1) * weight[:, None, None]
    return joined.reshape(mode_rows.shape)

def reference(probe_modes, patterns, specimen, offsets):
    detector = probe_modes.shape[-1]
    mode_count = probe_modes.shape[0]
    probe_field = lax.complex(probe_modes[:, 0], probe_modes[:, 1])
    probe_power = lax.optimization_barrier(jnp.sum(probe_modes[:, 0] ** 2 + probe_modes[:, 1] ** 2, axis=0))
    padded = jnp.pad(lax.complex(specimen[0], specimen[1]), ((detector, detector), (detector, detector)))
    frame_zeros = jnp.zeros(padded.shape, jnp.float32)
    mode_zeros = jnp.zeros((mode_count, detector, detector), jnp.float32)

    def one_position(position, running):
        grad_sum, light_sum, frame_num, frame_light, model_sum = running
        row_at = (offsets[position, 0] + detector).astype(jnp.int32)
        col_at = (offsets[position, 1] + detector).astype(jnp.int32)
        patch_now = lax.dynamic_slice(padded, (row_at, col_at), (detector, detector))
        exit_wave = probe_field * patch_now[None]
        model_sum = model_sum + jnp.sum(jnp.real(exit_wave) ** 2 + jnp.imag(exit_wave) ** 2)
        far_field = jnp.fft.fft2(exit_wave, norm='ortho')
        model_light = lax.optimization_barrier(jnp.sum(jnp.real(far_field) ** 2 + jnp.imag(far_field) ** 2, axis=0))
        factor = jnp.sqrt(patterns[position]) / jnp.sqrt(jnp.maximum(model_light, light_floor)) - 1.0
        change = jnp.fft.ifft2(far_field * factor[None], norm='ortho')
        grad_sum = grad_sum + jnp.conj(patch_now)[None] * change
        light_sum = light_sum + jnp.real(patch_now) ** 2 + jnp.imag(patch_now) ** 2
        contribution = lax.optimization_barrier(jnp.sum(jnp.conj(probe_field) * change, axis=0))
        old_num = lax.dynamic_slice(frame_num, (row_at, col_at), (detector, detector))
        frame_num = lax.dynamic_update_slice(frame_num, old_num + contribution, (row_at, col_at))
        old_light = lax.dynamic_slice(frame_light, (row_at, col_at), (detector, detector))
        frame_light = lax.dynamic_update_slice(frame_light, old_light + probe_power, (row_at, col_at))
        return (grad_sum, light_sum, frame_num, frame_light, model_sum)
    initial = (lax.complex(mode_zeros, mode_zeros), jnp.zeros((detector, detector), jnp.float32), lax.complex(frame_zeros, frame_zeros), frame_zeros, jnp.zeros((), jnp.float32))
    grad_sum, light_sum, frame_num, frame_light, model_sum = lax.fori_loop(0, POSITIONS, one_position, initial)
    interior_num = frame_num[detector:-detector, detector:-detector]
    interior_light = frame_light[detector:-detector, detector:-detector]
    new_field = padded[detector:-detector, detector:-detector] + interior_num / (interior_light + object_reg)
    new_specimen = jnp.stack([jnp.real(new_field), jnp.imag(new_field)])
    updated = probe_field + grad_sum / (light_sum + probe_reg)[None]
    updated_rows = jnp.stack([jnp.real(updated), jnp.imag(updated)], axis=1).reshape(2 * mode_count, -1)
    power_ratio = jnp.sum(patterns) / (model_sum + total_eps)
    gram_re, gram_im = gram_parts(updated_rows)
    new_rows = orthonormal_rows(updated_rows, gram_re, gram_im, power_ratio)
    return (new_rows.reshape(probe_modes.shape), new_specimen)
```

```python
import math

import jax
import jax.numpy as jnp
import numpy as np
from jax import lax
from jax.experimental import pallas as pl
from jax.experimental.pallas import tpu as pltpu
from jax.sharding import PartitionSpec as P

NS_STEPS = 8


highest = lax.Precision.HIGHEST
light_floor = 0.05
object_reg = 0.5
probe_reg = 1.0
total_eps = 1e-06


def extended_2(array, sides, width):
    for axis, dim in sides:
        size, length = (lax.axis_size(axis), array.shape[dim])
        up = [(i, (i + 1) % size) for i in range(size - 1)]
        down = [(j, i) for i, j in up]
        last = lax.slice_in_dim(array, length - width, length, axis=dim)
        first = lax.slice_in_dim(array, 0, width, axis=dim)
        before = lax.ppermute(last, axis, up)
        after = lax.ppermute(first, axis, down)
        array = jnp.concatenate([before, array, after], axis=dim)
    return array


def dft_tables(detector):
    indices = np.arange(detector, dtype=np.int64)
    angles = -2.0 * np.pi / detector * (indices[:, None] * indices[None, :] % detector)
    table_re = np.cos(angles) / np.sqrt(detector)
    table_im = np.sin(angles) / np.sqrt(detector)
    right = np.block([[table_re, table_im], [-table_im, table_re]]).astype(np.float32)
    left = np.ascontiguousarray(right.T)
    parts = []
    for table in (right, left):
        high = table.astype(jnp.bfloat16)
        low = (table - high.astype(np.float32)).astype(jnp.bfloat16)
        parts.append((high, low))
    (rh, rl), (lh, ll) = parts
    return (
        np.concatenate([rh, rl, rh], axis=0),
        np.concatenate([lh, ll, lh], axis=1),
        np.concatenate([rh, rl, rh], axis=1),
        np.concatenate([lh, ll, lh], axis=0),
    )


def halves(value):
    high = value.astype(jnp.bfloat16)
    low = (value - high.astype(jnp.float32)).astype(jnp.bfloat16)
    return high, low


def scan_kernel(
    offs, probe, patterns, extended, right_f, left_f, left_b, right_b,
    grad, light, frame_out, total_out,
    ext, frame, deep, half, far, power,
    *, block_rows, block_cols,
):
    modes = probe.shape[0]
    det = probe.shape[-1]
    count = patterns.shape[0]
    col_blocks = extended.shape[2] // det
    f32 = jnp.float32
    row_base = lax.axis_index("scan") * block_rows - det
    col_base = lax.axis_index("tile") * block_cols - det
    lanes = lax.broadcasted_iota(jnp.int32, (det, det), 1)
    for c in range(2):
        for j in range(col_blocks):
            ext[c, j] = extended[c, :, j * det : (j + 1) * det]
        ext[c, col_blocks] = jnp.zeros_like(ext[c, col_blocks])
    frame[...] = jnp.zeros_like(frame)
    grad[...] = jnp.zeros_like(grad)
    light[...] = jnp.zeros_like(light)
    acc = jnp.zeros((det, det), f32)
    for k in range(modes):
        acc = acc + probe[k, 0] * probe[k, 0] + probe[k, 1] * probe[k, 1]
    power[...] = acc

    def one(p, total):
        row = offs[p, 0] - row_base
        col = offs[p, 1] - col_base
        block = col // det
        shift = col - block * det
        back = lax.rem(det - shift, det)
        rows = pl.ds(row, det)

        def patch_part(c):
            first = pltpu.roll(ext[c, block, rows, :], back, 1)
            second = pltpu.roll(ext[c, block + 1, rows, :], back, 1)
            return jnp.where(lanes < det - shift, first, second)

        patch_re = patch_part(0)
        patch_im = patch_part(1)
        patch_light = patch_re * patch_re + patch_im * patch_im
        light[...] = light[...] + patch_light
        total = total + patch_light * power[...]
        for k in range(modes):
            at = pl.ds(k * det, det)
            pr, pi = probe[k, 0], probe[k, 1]
            for c, value in enumerate((pr * patch_re - pi * patch_im, pr * patch_im + pi * patch_re)):
                high, low = halves(value)
                deep[at, pl.ds(c * det, det)] = high
                deep[at, pl.ds((2 + c) * det, det)] = high
                deep[at, pl.ds((4 + c) * det, det)] = low
        half[...] = jnp.dot(deep[...], right_f[...], preferred_element_type=f32)
        model = jnp.zeros((det, det), f32)
        for k in range(0, modes, 2):
            lo_at, hi_at = pl.ds(k * det, det), pl.ds((k + 1) * det, det)
            first, second = half[lo_at, :], half[hi_at, :]
            paired = jnp.concatenate(
                [
                    jnp.concatenate([first[:, :det], second[:, :det]], axis=1),
                    jnp.concatenate([first[:, det:], second[:, det:]], axis=1),
                ],
                axis=0,
            )
            high, low = halves(paired)
            stacked = jnp.concatenate([high, high, low], axis=0)
            out = jnp.dot(left_f[...], stacked, preferred_element_type=f32)
            far[:, pl.ds(k * det, 2 * det)] = out
            squares = out * out
            both = squares[:det] + squares[det:]
            model = model + both[:, :det] + both[:, det:]
        factor = jnp.sqrt(patterns[p]) / jnp.sqrt(jnp.maximum(model, light_floor)) - 1.0
        wide = jnp.concatenate([factor, factor], axis=1)
        wide = jnp.concatenate([wide, wide], axis=0)
        for k in range(0, modes, 2):
            high, low = halves(far[:, pl.ds(k * det, 2 * det)] * wide)
            stacked = jnp.concatenate([high, high, low], axis=0)
            out = jnp.dot(left_b[...], stacked, preferred_element_type=f32)
            high, low = halves(out)
            for m in range(2):
                at = pl.ds((k + m) * det, det)
                for c in range(2):
                    part_h = high[c * det : (c + 1) * det, m * det : (m + 1) * det]
                    part_l = low[c * det : (c + 1) * det, m * det : (m + 1) * det]
                    deep[at, pl.ds(c * det, det)] = part_h
                    deep[at, pl.ds((2 + c) * det, det)] = part_h
                    deep[at, pl.ds((4 + c) * det, det)] = part_l
        half[...] = jnp.dot(deep[...], right_b[...], preferred_element_type=f32)
        num_re = jnp.zeros((det, det), f32)
        num_im = jnp.zeros((det, det), f32)
        for k in range(modes):
            at = pl.ds(k * det, det)
            cr, ci = half[at, :det], half[at, det:]
            pr, pi = probe[k, 0], probe[k, 1]
            grad[0, k] = grad[0, k] + patch_re * cr + patch_im * ci
            grad[1, k] = grad[1, k] + patch_re * ci - patch_im * cr
            num_re = num_re + pr * cr + pi * ci
            num_im = num_im + pr * ci - pi * cr
        zero = jnp.zeros((det, det), f32)
        for c, value in enumerate((num_re, num_im, power[...])):
            turned = pltpu.roll(value, shift, 1)
            frame[c, block, rows, :] = frame[c, block, rows, :] + jnp.where(lanes >= shift, turned, zero)
            frame[c, block + 1, rows, :] = frame[c, block + 1, rows, :] + jnp.where(lanes < shift, turned, zero)
        return total

    total_out[...] = lax.fori_loop(0, count, one, jnp.zeros((det, det), f32))
    for c in range(3):
        for j in range(col_blocks):
            frame_out[c, :, j * det : (j + 1) * det] = frame[c, j]


def scan_positions(offsets, probe_modes, patterns, extended, block_rows, block_cols):
    modes, _, det, _ = probe_modes.shape
    f32 = jnp.float32
    ext_rows, ext_cols = extended.shape[1:]
    col_blocks = ext_cols // det
    vmem = pl.BlockSpec(memory_space=pltpu.VMEM)
    tables = [jnp.asarray(t) for t in dft_tables(det)]

    def kernel(*refs):
        scan_kernel(*refs, block_rows=block_rows, block_cols=block_cols)

    return pl.pallas_call(
        kernel,
        name="scan_positions",
        out_shape=(
            jax.ShapeDtypeStruct((2, modes, det, det), f32),
            jax.ShapeDtypeStruct((det, det), f32),
            jax.ShapeDtypeStruct((3, ext_rows, ext_cols), f32),
            jax.ShapeDtypeStruct((det, det), f32),
        ),
        in_specs=[pl.BlockSpec(memory_space=pltpu.SMEM)] + [vmem] * 7,
        out_specs=(vmem,) * 4,
        scratch_shapes=[
            pltpu.VMEM((2, col_blocks + 1, ext_rows, det), f32),
            pltpu.VMEM((3, col_blocks + 1, ext_rows, det), f32),
            pltpu.VMEM((modes * det, 6 * det), jnp.bfloat16),
            pltpu.VMEM((modes * det, 2 * det), f32),
            pltpu.VMEM((2 * det, modes * det), f32),
            pltpu.VMEM((det, det), f32),
        ],
        compiler_params=pltpu.CompilerParams(vmem_limit_bytes=48 * 1024 * 1024),
    )(offsets, probe_modes, patterns, extended, *tables)


def newton_steps(gram_re, gram_im):
    mode_count = gram_re.shape[0]
    upper = jnp.concatenate([gram_re, -gram_im], axis=1)
    lower = jnp.concatenate([gram_im, gram_re], axis=1)
    embedded = jnp.concatenate([upper, lower], axis=0)
    frobenius = jnp.sqrt(jnp.sum(embedded * embedded))
    identity = jnp.eye(2 * mode_count, dtype=jnp.float32)
    current = embedded / frobenius
    inverse = identity
    for repeat in range(NS_STEPS):
        factor = 1.5 * identity - 0.5 * jnp.dot(
            inverse, current, precision=highest, preferred_element_type=jnp.float32
        )
        current = jnp.dot(current, factor, precision=highest, preferred_element_type=jnp.float32)
        inverse = jnp.dot(factor, inverse, precision=highest, preferred_element_type=jnp.float32)
    inverse = inverse / jnp.sqrt(frobenius)
    return (inverse[:mode_count, :mode_count], inverse[mode_count:, :mode_count])


def gram_parts(mode_rows):
    real_rows = mode_rows[: mode_rows.shape[0] // 2]
    imag_rows = mode_rows[mode_rows.shape[0] // 2 :]
    gram_re = jnp.dot(
        real_rows, real_rows.T, precision=highest, preferred_element_type=jnp.float32
    ) + jnp.dot(imag_rows, imag_rows.T, precision=highest, preferred_element_type=jnp.float32)
    gram_im = jnp.dot(
        real_rows, imag_rows.T, precision=highest, preferred_element_type=jnp.float32
    ) - jnp.dot(imag_rows, real_rows.T, precision=highest, preferred_element_type=jnp.float32)
    return (gram_re, gram_im)


def orthonormal_rows(mode_rows, gram_re, gram_im, power_ratio):
    real_rows = mode_rows[: mode_rows.shape[0] // 2]
    imag_rows = mode_rows[mode_rows.shape[0] // 2 :]
    mix_re, mix_im = newton_steps(gram_re, gram_im)
    ortho_re = jnp.dot(
        mix_re.T, real_rows, precision=highest, preferred_element_type=jnp.float32
    ) - jnp.dot(mix_im.T, imag_rows, precision=highest, preferred_element_type=jnp.float32)
    ortho_im = jnp.dot(
        mix_im.T, real_rows, precision=highest, preferred_element_type=jnp.float32
    ) + jnp.dot(mix_re.T, imag_rows, precision=highest, preferred_element_type=jnp.float32)
    weight = jnp.sqrt(power_ratio * jnp.diagonal(gram_re))
    return jnp.stack([ortho_re, ortho_im], axis=1) * weight[:, None, None]


def fold_interior(frame_sum, folded, detector, block_rows, block_cols):
    rows_end = block_rows + 3 * detector
    cols_end = block_cols + 3 * detector
    centre_rows = slice(2 * detector, 2 * detector + block_rows)
    centre_cols = slice(2 * detector, 2 * detector + block_cols)
    interior = frame_sum[:, detector : detector + block_rows, detector : detector + block_cols]
    interior = interior.at[:, :detector, :].add(folded[:, :detector, centre_cols])
    interior = interior.at[:, block_rows - detector :, :].add(folded[:, rows_end:, centre_cols])
    interior = interior.at[:, :, :detector].add(folded[:, centre_rows, :detector])
    interior = interior.at[:, :, block_cols - detector :].add(folded[:, centre_rows, cols_end:])
    interior = interior.at[:, :detector, :detector].add(folded[:, :detector, :detector])
    interior = interior.at[:, :detector, block_cols - detector :].add(
        folded[:, :detector, cols_end:]
    )
    interior = interior.at[:, block_rows - detector :, :detector].add(
        folded[:, rows_end:, :detector]
    )
    interior = interior.at[:, block_rows - detector :, block_cols - detector :].add(
        folded[:, rows_end:, cols_end:]
    )
    return interior


def body(probe_modes, patterns, specimen, offsets):
    detector = probe_modes.shape[-1]
    mode_count = probe_modes.shape[0]
    block_rows = specimen.shape[1]
    block_cols = specimen.shape[2]
    extended = extended_2(specimen, (("scan", 1), ("tile", 2)), detector)
    grad, light_sum, frame_sum, model_grid = scan_positions(
        offsets, probe_modes, patterns, extended, block_rows, block_cols
    )
    pixels = detector * detector
    totals = jnp.stack([jnp.sum(patterns, axis=(0, 1)), jnp.sum(model_grid, axis=0)])
    packed = jnp.concatenate(
        [
            grad.reshape(2 * mode_count * detector, detector),
            light_sum,
            jnp.pad(totals, ((0, 6), (0, 0))),
        ],
        axis=0,
    )
    summed = lax.psum(packed, ("scan", "tile"))
    rows_grad = 2 * mode_count * detector
    grad_total = summed[:rows_grad].reshape(2 * mode_count, pixels)
    light_total = summed[rows_grad : rows_grad + detector].reshape(1, pixels)
    measured_all = jnp.sum(summed[rows_grad + detector])
    model_all = jnp.sum(summed[rows_grad + detector + 1])
    power_ratio = measured_all / (model_all + total_eps)
    folded = extended_2(frame_sum, (("scan", 1), ("tile", 2)), detector)
    interior = fold_interior(frame_sum, folded, detector, block_rows, block_cols)
    new_specimen = specimen + interior[0:2] / (interior[2] + object_reg)[None]
    probe_rows = jnp.swapaxes(probe_modes, 0, 1).reshape(2 * mode_count, pixels)
    updated = probe_rows + grad_total / (light_total + probe_reg)
    gram_re, gram_im = gram_parts(updated)
    new_probe = orthonormal_rows(updated, gram_re, gram_im, power_ratio).reshape(probe_modes.shape)
    return (new_probe, new_specimen)


def solution(mesh):
    return jax.shard_map(
        body,
        mesh=mesh,
        in_specs=(
            P(),
            P(("scan", "tile"), None, None),
            P(None, "scan", "tile"),
            P(("scan", "tile"), None),
        ),
        out_specs=(P(), P(None, "scan", "tile")),
        check_vma=False,
    )
```

```python
import math

import jax
import jax.numpy as jnp
import numpy as np
from jax import lax
from jax.experimental import pallas as pl
from jax.experimental.pallas import tpu as pltpu
from jax.sharding import PartitionSpec as P

NS_STEPS = 8


highest = lax.Precision.HIGHEST
light_floor = 0.05
object_reg = 0.5
probe_reg = 1.0
total_eps = 1e-06


def extended_2(array, sides, width):
    for axis, dim in sides:
        size, length = (lax.axis_size(axis), array.shape[dim])
        up = [(i, (i + 1) % size) for i in range(size - 1)]
        down = [(j, i) for i, j in up]
        last = lax.slice_in_dim(array, length - width, length, axis=dim)
        first = lax.slice_in_dim(array, 0, width, axis=dim)
        before = lax.ppermute(last, axis, up)
        after = lax.ppermute(first, axis, down)
        array = jnp.concatenate([before, array, after], axis=dim)
    return array


def dft_tables(detector):
    indices = np.arange(detector, dtype=np.int64)
    angles = -2.0 * np.pi / detector * (indices[:, None] * indices[None, :] % detector)
    table_re = np.cos(angles) / np.sqrt(detector)
    table_im = np.sin(angles) / np.sqrt(detector)
    right = np.block([[table_re, table_im], [-table_im, table_re]]).astype(np.float32)
    left = np.ascontiguousarray(right.T)
    parts = []
    for table in (right, left):
        high = table.astype(jnp.bfloat16)
        low = (table - high.astype(np.float32)).astype(jnp.bfloat16)
        parts.append((high, low))
    (rh, rl), (lh, ll) = parts
    return (
        np.concatenate([rh, rl, rh], axis=0),
        np.concatenate([lh, ll, lh], axis=1),
        np.concatenate([rh, rl, rh], axis=1),
        np.concatenate([lh, ll, lh], axis=0),
    )


def halves(value):
    high = value.astype(jnp.bfloat16)
    low = (value - high.astype(jnp.float32)).astype(jnp.bfloat16)
    return high, low


def scan_kernel(
    offs, probe, patterns, extended, right_f, left_f, left_b, right_b,
    packed, frame_out,
    ext, frame, deep, half, far, power, grad, light,
    *, block_rows, block_cols,
):
    modes = probe.shape[0]
    det = probe.shape[-1]
    count = patterns.shape[0]
    col_blocks = extended.shape[2] // det
    f32 = jnp.float32
    row_base = lax.axis_index("scan") * block_rows - det
    col_base = lax.axis_index("tile") * block_cols - det
    lanes = lax.broadcasted_iota(jnp.int32, (det, det), 1)
    for c in range(2):
        for j in range(col_blocks):
            ext[c, j] = extended[c, :, j * det : (j + 1) * det]
        ext[c, col_blocks] = jnp.zeros_like(ext[c, col_blocks])
    frame[...] = jnp.zeros_like(frame)
    grad[...] = jnp.zeros_like(grad)
    light[...] = jnp.zeros_like(light)
    acc = jnp.zeros((det, det), f32)
    for k in range(modes):
        acc = acc + probe[k, 0] * probe[k, 0] + probe[k, 1] * probe[k, 1]
    power[...] = acc

    def one(p, total):
        row = offs[p, 0] - row_base
        col = offs[p, 1] - col_base
        block = col // det
        shift = col - block * det
        back = lax.rem(det - shift, det)
        rows = pl.ds(row, det)

        def patch_part(c):
            first = pltpu.roll(ext[c, block, rows, :], back, 1)
            second = pltpu.roll(ext[c, block + 1, rows, :], back, 1)
            return jnp.where(lanes < det - shift, first, second)

        patch_re = patch_part(0)
        patch_im = patch_part(1)
        patch_light = patch_re * patch_re + patch_im * patch_im
        light[...] = light[...] + patch_light
        total = total + patch_light * power[...]
        for k in range(modes):
            at = pl.ds(k * det, det)
            pr, pi = probe[k, 0], probe[k, 1]
            for c, value in enumerate((pr * patch_re - pi * patch_im, pr * patch_im + pi * patch_re)):
                high, low = halves(value)
                deep[at, pl.ds(c * det, det)] = high
                deep[at, pl.ds((2 + c) * det, det)] = high
                deep[at, pl.ds((4 + c) * det, det)] = low
        half[...] = jnp.dot(deep[...], right_f[...], preferred_element_type=f32)
        model = jnp.zeros((det, det), f32)
        for k in range(0, modes, 2):
            lo_at, hi_at = pl.ds(k * det, det), pl.ds((k + 1) * det, det)
            first, second = half[lo_at, :], half[hi_at, :]
            paired = jnp.concatenate(
                [
                    jnp.concatenate([first[:, :det], second[:, :det]], axis=1),
                    jnp.concatenate([first[:, det:], second[:, det:]], axis=1),
                ],
                axis=0,
            )
            high, low = halves(paired)
            stacked = jnp.concatenate([high, high, low], axis=0)
            out = jnp.dot(left_f[...], stacked, preferred_element_type=f32)
            far[:, pl.ds(k * det, 2 * det)] = out
            squares = out * out
            both = squares[:det] + squares[det:]
            model = model + both[:, :det] + both[:, det:]
        factor = jnp.sqrt(patterns[p]) / jnp.sqrt(jnp.maximum(model, light_floor)) - 1.0
        wide = jnp.concatenate([factor, factor], axis=1)
        wide = jnp.concatenate([wide, wide], axis=0)
        for k in range(0, modes, 2):
            high, low = halves(far[:, pl.ds(k * det, 2 * det)] * wide)
            stacked = jnp.concatenate([high, high, low], axis=0)
            out = jnp.dot(left_b[...], stacked, preferred_element_type=f32)
            high, low = halves(out)
            for m in range(2):
                at = pl.ds((k + m) * det, det)
                for c in range(2):
                    part_h = high[c * det : (c + 1) * det, m * det : (m + 1) * det]
                    part_l = low[c * det : (c + 1) * det, m * det : (m + 1) * det]
                    deep[at, pl.ds(c * det, det)] = part_h
                    deep[at, pl.ds((2 + c) * det, det)] = part_h
                    deep[at, pl.ds((4 + c) * det, det)] = part_l
        half[...] = jnp.dot(deep[...], right_b[...], preferred_element_type=f32)
        num_re = jnp.zeros((det, det), f32)
        num_im = jnp.zeros((det, det), f32)
        for k in range(modes):
            at = pl.ds(k * det, det)
            cr, ci = half[at, :det], half[at, det:]
            pr, pi = probe[k, 0], probe[k, 1]
            grad[0, k] = grad[0, k] + patch_re * cr + patch_im * ci
            grad[1, k] = grad[1, k] + patch_re * ci - patch_im * cr
            num_re = num_re + pr * cr + pi * ci
            num_im = num_im + pr * ci - pi * cr
        zero = jnp.zeros((det, det), f32)
        for c, value in enumerate((num_re, num_im, power[...])):
            turned = pltpu.roll(value, shift, 1)
            frame[c, block, rows, :] = frame[c, block, rows, :] + jnp.where(lanes >= shift, turned, zero)
            frame[c, block + 1, rows, :] = frame[c, block + 1, rows, :] + jnp.where(lanes < shift, turned, zero)
        return total

    model_grid = lax.fori_loop(0, count, one, jnp.zeros((det, det), f32))
    measured = jnp.zeros((det, det), f32)
    for p in range(count):
        measured = measured + patterns[p]
    tiles = det // 8
    for k in range(2 * modes):
        packed[k * tiles : (k + 1) * tiles] = grad[k // modes, k % modes].reshape(tiles, 8, det)
    last = 2 * modes * tiles
    packed[last : last + tiles] = light[...].reshape(tiles, 8, det)
    packed[last + tiles] = jnp.sum(measured.reshape(tiles, 8, det), axis=0)
    packed[last + tiles + 1] = jnp.sum(model_grid.reshape(tiles, 8, det), axis=0)
    for extra in range(last + tiles + 2, packed.shape[0]):
        packed[extra] = jnp.zeros((8, det), f32)
    for c in range(3):
        for j in range(col_blocks):
            frame_out[c, :, j * det : (j + 1) * det] = frame[c, j]


def scan_positions(offsets, probe_modes, patterns, extended, block_rows, block_cols):
    modes, _, det, _ = probe_modes.shape
    f32 = jnp.float32
    ext_rows, ext_cols = extended.shape[1:]
    col_blocks = ext_cols // det
    vmem = pl.BlockSpec(memory_space=pltpu.VMEM)
    tables = [jnp.asarray(t) for t in dft_tables(det)]

    def kernel(*refs):
        scan_kernel(*refs, block_rows=block_rows, block_cols=block_cols)

    return pl.pallas_call(
        kernel,
        name="scan_positions",
        out_shape=(
            jax.ShapeDtypeStruct((packed_tiles(modes, det), 8, det), f32),
            jax.ShapeDtypeStruct((3, ext_rows, ext_cols), f32),
        ),
        in_specs=[pl.BlockSpec(memory_space=pltpu.SMEM)] + [vmem] * 7,
        out_specs=(vmem,) * 2,
        scratch_shapes=[
            pltpu.VMEM((2, col_blocks + 1, ext_rows, det), f32),
            pltpu.VMEM((3, col_blocks + 1, ext_rows, det), f32),
            pltpu.VMEM((modes * det, 6 * det), jnp.bfloat16),
            pltpu.VMEM((modes * det, 2 * det), f32),
            pltpu.VMEM((2 * det, modes * det), f32),
            pltpu.VMEM((det, det), f32),
            pltpu.VMEM((2, modes, det, det), f32),
            pltpu.VMEM((det, det), f32),
        ],
        compiler_params=pltpu.CompilerParams(vmem_limit_bytes=48 * 1024 * 1024),
    )(offsets, probe_modes, patterns, extended, *tables)


def newton_steps(gram_re, gram_im):
    mode_count = gram_re.shape[0]
    upper = jnp.concatenate([gram_re, -gram_im], axis=1)
    lower = jnp.concatenate([gram_im, gram_re], axis=1)
    embedded = jnp.concatenate([upper, lower], axis=0)
    frobenius = jnp.sqrt(jnp.sum(embedded * embedded))
    identity = jnp.eye(2 * mode_count, dtype=jnp.float32)
    current = embedded / frobenius
    inverse = identity
    for repeat in range(NS_STEPS):
        factor = 1.5 * identity - 0.5 * jnp.dot(
            inverse, current, precision=highest, preferred_element_type=jnp.float32
        )
        current = jnp.dot(current, factor, precision=highest, preferred_element_type=jnp.float32)
        inverse = jnp.dot(factor, inverse, precision=highest, preferred_element_type=jnp.float32)
    inverse = inverse / jnp.sqrt(frobenius)
    return (inverse[:mode_count, :mode_count], inverse[mode_count:, :mode_count])


def gram_parts(mode_rows):
    real_rows = mode_rows[: mode_rows.shape[0] // 2]
    imag_rows = mode_rows[mode_rows.shape[0] // 2 :]
    gram_re = jnp.dot(
        real_rows, real_rows.T, precision=highest, preferred_element_type=jnp.float32
    ) + jnp.dot(imag_rows, imag_rows.T, precision=highest, preferred_element_type=jnp.float32)
    gram_im = jnp.dot(
        real_rows, imag_rows.T, precision=highest, preferred_element_type=jnp.float32
    ) - jnp.dot(imag_rows, real_rows.T, precision=highest, preferred_element_type=jnp.float32)
    return (gram_re, gram_im)


def orthonormal_rows(mode_rows, gram_re, gram_im, power_ratio):
    real_rows = mode_rows[: mode_rows.shape[0] // 2]
    imag_rows = mode_rows[mode_rows.shape[0] // 2 :]
    mix_re, mix_im = newton_steps(gram_re, gram_im)
    ortho_re = jnp.dot(
        mix_re.T, real_rows, precision=highest, preferred_element_type=jnp.float32
    ) - jnp.dot(mix_im.T, imag_rows, precision=highest, preferred_element_type=jnp.float32)
    ortho_im = jnp.dot(
        mix_im.T, real_rows, precision=highest, preferred_element_type=jnp.float32
    ) + jnp.dot(mix_re.T, imag_rows, precision=highest, preferred_element_type=jnp.float32)
    weight = jnp.sqrt(power_ratio * jnp.diagonal(gram_re))
    return jnp.stack([ortho_re, ortho_im], axis=1) * weight[:, None, None]


fast_bits = (("scan", 1), ("scan", 2), ("scan", 4), ("tile", 1))
halvings = 3


def packed_tiles(modes, det):
    tiles = (2 * modes + 1) * (det // 8) + 2
    step = len(fast_bits) * 2**halvings
    return -(-tiles // step) * step


def mesh_bits():
    bits = list(fast_bits)
    for axis in ("scan", "tile"):
        bit = 1
        while bit < lax.axis_size(axis):
            if (axis, bit) not in bits:
                bits.append((axis, bit))
            bit *= 2
    return bits


def directions():
    return [(i, j) for i, j in ((1, 0), (-1, 0), (0, 1), (0, -1), (1, 1), (1, -1), (-1, 1), (-1, -1))]


def exchange_kernel(bits, packed, frame, out, interior, acc, landing, *rest):
    slots = rest[:8]
    send_sem, recv_sem, fold_send, fold_recv = rest[8:]
    pieces = len(fast_bits)
    piece = packed.shape[0] // pieces
    det = (frame.shape[1] - interior.shape[1]) // 2
    block_rows, block_cols = interior.shape[1:]
    here = {axis: lax.axis_index(axis) for axis in ("scan", "tile")}
    sizes = {axis: lax.axis_size(axis) for axis in ("scan", "tile")}

    def digit(axis, bit):
        return (here[axis] // bit) % 2

    def partner(axis, bit):
        return {axis: here[axis] + bit * (1 - 2 * digit(axis, bit))}

    def copy(src, dst, g, step, axis, bit):
        return pltpu.make_async_remote_copy(
            src_ref=src, dst_ref=dst, send_sem=send_sem.at[g, step], recv_sem=recv_sem.at[g, step],
            device_id=partner(axis, bit), device_id_type=pl.DeviceIdType.MESH,
        )

    plans = []
    for g in range(pieces):
        order = [fast_bits[(g + i) % pieces] for i in range(pieces)] + bits[pieces:]
        steps = []
        start, size, land = g * piece, piece, 0
        for axis, bit in order[:halvings]:
            size //= 2
            mine = digit(axis, bit)
            keep, give = start + mine * size, start + (1 - mine) * size
            steps.append(("halve", axis, bit, give, keep, size, land))
            start = keep
            land += size
        for axis, bit in order[halvings:]:
            steps.append(("both", axis, bit, start, start, size, land))
            land += size
        for axis, bit in reversed(order[:halvings]):
            low = start - digit(axis, bit) * size
            steps.append(("gather", axis, bit, start, low + (1 - digit(axis, bit)) * size, size, land))
            start = low
            land += size
            size *= 2
        plans.append(steps)
    total = len(plans[0])

    def make(g, step):
        kind, axis, bit, give, keep, size, land = plans[g][step]
        source = packed if step == 0 else acc
        src = source.at[pl.ds(give, size)]
        return copy(src, landing.at[g, pl.ds(land, size)], g, step, axis, bit)

    def settle(g, step):
        kind, axis, bit, give, keep, size, land = plans[g][step]
        source = packed if step == 0 else acc
        arrived = landing[g, pl.ds(land, size)]
        acc[pl.ds(keep, size)] = arrived if kind == "gather" else source[pl.ds(keep, size)] + arrived

    def span(shift, block):
        low = {-1: 0, 0: det, 1: det + block}[shift]
        return pl.ds(low, block if shift == 0 else det)

    def inner(shift, block):
        low = {-1: block - det, 0: 0, 1: 0}[shift]
        return pl.ds(low, block if shift == 0 else det)

    def valid(shift_rows, shift_cols):
        row, col = here["scan"] + shift_rows, here["tile"] + shift_cols
        return (row >= 0) & (row < sizes["scan"]) & (col >= 0) & (col < sizes["tile"])

    def fold(index):
        shift_rows, shift_cols = directions()[index]
        return pltpu.make_async_remote_copy(
            src_ref=frame.at[:, span(shift_rows, block_rows), span(shift_cols, block_cols)],
            dst_ref=slots[index],
            send_sem=fold_send.at[index],
            recv_sem=fold_recv.at[index],
            device_id={
                "scan": (here["scan"] + shift_rows + sizes["scan"]) % sizes["scan"],
                "tile": (here["tile"] + shift_cols + sizes["tile"]) % sizes["tile"],
            },
            device_id_type=pl.DeviceIdType.MESH,
        )

    def fold_start(indices):
        for index in indices:
            @pl.when(valid(*directions()[index]))
            def _():
                fold(index).start()

    interior[...] = frame[:, det : det + block_rows, det : det + block_cols]
    for g in range(pieces):
        make(g, 0).start()
    fold_start((0, 1))
    for step in range(total):
        for g in range(pieces):
            make(g, step).wait()
            settle(g, step)
            if step + 1 < total:
                make(g, step + 1).start()
        if step == 0:
            fold_start((2, 3))
        if step == 1:
            fold_start((4, 5, 6, 7))
    out[...] = acc[...]
    for index, (shift_rows, shift_cols) in enumerate(directions()):
        @pl.when(valid(shift_rows, shift_cols))
        def _():
            fold(index).wait_send()

        @pl.when(valid(-shift_rows, -shift_cols))
        def _():
            fold(index).wait_recv()
            rows, cols = inner(shift_rows, block_rows), inner(shift_cols, block_cols)
            interior[:, rows, cols] = interior[:, rows, cols] + slots[index][...]


def exchange(packed, frame, det, block_rows, block_cols):
    f32 = jnp.float32
    bits = mesh_bits()
    pieces = len(fast_bits)
    piece = packed.shape[0] // pieces
    steps = len(bits) + halvings
    small = piece // 2**halvings
    land = 2 * (piece - small) + (len(bits) - halvings) * small
    vmem = pl.BlockSpec(memory_space=pltpu.VMEM)
    slots = [
        pltpu.VMEM((3, det if i else block_rows, det if j else block_cols), f32) for i, j in directions()
    ]

    def kernel(*refs):
        exchange_kernel(bits, *refs)

    return pl.pallas_call(
        kernel,
        name="exchange",
        out_shape=(
            jax.ShapeDtypeStruct(packed.shape, f32),
            jax.ShapeDtypeStruct((3, block_rows, block_cols), f32),
        ),
        in_specs=[vmem, vmem],
        out_specs=(vmem, vmem),
        scratch_shapes=[
            pltpu.VMEM(packed.shape, f32),
            pltpu.VMEM((pieces, land) + packed.shape[1:], f32),
            *slots,
            pltpu.SemaphoreType.DMA((pieces, steps)),
            pltpu.SemaphoreType.DMA((pieces, steps)),
            pltpu.SemaphoreType.DMA((8,)),
            pltpu.SemaphoreType.DMA((8,)),
        ],
        compiler_params=pltpu.CompilerParams(has_side_effects=True, vmem_limit_bytes=40 * 1024 * 1024),
    )(packed, frame)


def body(probe_modes, patterns, specimen, offsets):
    detector = probe_modes.shape[-1]
    mode_count = probe_modes.shape[0]
    block_rows = specimen.shape[1]
    block_cols = specimen.shape[2]
    extended = extended_2(specimen, (("scan", 1), ("tile", 2)), detector)
    packed, frame_sum = scan_positions(
        offsets, probe_modes, patterns, extended, block_rows, block_cols
    )
    summed, interior = exchange(packed, frame_sum, detector, block_rows, block_cols)
    pixels = detector * detector
    tiles = detector // 8
    last = 2 * mode_count * tiles
    grad_total = summed[:last].reshape(2 * mode_count, pixels)
    light_total = summed[last : last + tiles].reshape(1, pixels)
    measured_all = jnp.sum(summed[last + tiles])
    model_all = jnp.sum(summed[last + tiles + 1])
    power_ratio = measured_all / (model_all + total_eps)
    new_specimen = specimen + interior[0:2] / (interior[2] + object_reg)[None]
    probe_rows = jnp.swapaxes(probe_modes, 0, 1).reshape(2 * mode_count, pixels)
    updated = probe_rows + grad_total / (light_total + probe_reg)
    gram_re, gram_im = gram_parts(updated)
    new_probe = orthonormal_rows(updated, gram_re, gram_im, power_ratio).reshape(probe_modes.shape)
    return (new_probe, new_specimen)


def solution(mesh):
    return jax.shard_map(
        body,
        mesh=mesh,
        in_specs=(
            P(),
            P(("scan", "tile"), None, None),
            P(None, "scan", "tile"),
            P(("scan", "tile"), None),
        ),
        out_specs=(P(), P(None, "scan", "tile")),
        check_vma=False,
    )
```

```python
import math

import jax
import jax.numpy as jnp
import numpy as np
from jax import lax
from jax.experimental import pallas as pl
from jax.experimental.pallas import tpu as pltpu
from jax.sharding import PartitionSpec as P

NS_STEPS = 8


highest = lax.Precision.HIGHEST
light_floor = 0.05
object_reg = 0.5
probe_reg = 1.0
total_eps = 1e-06


def dft_tables(detector):
    indices = np.arange(detector, dtype=np.int64)
    angles = -2.0 * np.pi / detector * (indices[:, None] * indices[None, :] % detector)
    table_re = np.cos(angles) / np.sqrt(detector)
    table_im = np.sin(angles) / np.sqrt(detector)
    right = np.block([[table_re, table_im], [-table_im, table_re]]).astype(np.float32)
    left = np.ascontiguousarray(right.T)
    parts = []
    for table in (right, left):
        high = table.astype(jnp.bfloat16)
        low = (table - high.astype(np.float32)).astype(jnp.bfloat16)
        parts.append((high, low))
    (rh, rl), (lh, ll) = parts
    return (
        np.concatenate([rh, rl, rh], axis=0),
        np.concatenate([lh, ll, lh], axis=1),
        np.concatenate([rh, rl, rh], axis=1),
        np.concatenate([lh, ll, lh], axis=0),
    )


def halves(value):
    high = value.astype(jnp.bfloat16)
    low = (value - high.astype(jnp.float32)).astype(jnp.bfloat16)
    return high, low


def scan_kernel(
    offs, probe, patterns, extended, right_f, left_f, left_b, right_b,
    packed, frame_out,
    ext, frame, deep, half, far, power, grad, light,
    *, block_rows, block_cols,
):
    modes = probe.shape[0]
    det = probe.shape[-1]
    count = patterns.shape[0]
    col_blocks = extended.shape[2] // det
    f32 = jnp.float32
    row_base = lax.axis_index("scan") * block_rows - det
    col_base = lax.axis_index("tile") * block_cols - det
    lanes = lax.broadcasted_iota(jnp.int32, (det, det), 1)
    for c in range(2):
        for j in range(col_blocks):
            ext[c, j] = extended[c, :, j * det : (j + 1) * det]
        ext[c, col_blocks] = jnp.zeros_like(ext[c, col_blocks])
    frame[...] = jnp.zeros_like(frame)
    grad[...] = jnp.zeros_like(grad)
    light[...] = jnp.zeros_like(light)
    acc = jnp.zeros((det, det), f32)
    for k in range(modes):
        acc = acc + probe[k, 0] * probe[k, 0] + probe[k, 1] * probe[k, 1]
    power[...] = acc

    def one(p, total):
        row = offs[p, 0] - row_base
        col = offs[p, 1] - col_base
        block = col // det
        shift = col - block * det
        back = lax.rem(det - shift, det)
        rows = pl.ds(row, det)

        def patch_part(c):
            first = pltpu.roll(ext[c, block, rows, :], back, 1)
            second = pltpu.roll(ext[c, block + 1, rows, :], back, 1)
            return jnp.where(lanes < det - shift, first, second)

        patch_re = patch_part(0)
        patch_im = patch_part(1)
        patch_light = patch_re * patch_re + patch_im * patch_im
        light[...] = light[...] + patch_light
        total = total + patch_light * power[...]
        for k in range(modes):
            at = pl.ds(k * det, det)
            pr, pi = probe[k, 0], probe[k, 1]
            for c, value in enumerate((pr * patch_re - pi * patch_im, pr * patch_im + pi * patch_re)):
                high, low = halves(value)
                deep[at, pl.ds(c * det, det)] = high
                deep[at, pl.ds((2 + c) * det, det)] = high
                deep[at, pl.ds((4 + c) * det, det)] = low
        half[...] = jnp.dot(deep[...], right_f[...], preferred_element_type=f32)
        model = jnp.zeros((det, det), f32)
        for k in range(0, modes, 2):
            lo_at, hi_at = pl.ds(k * det, det), pl.ds((k + 1) * det, det)
            first, second = half[lo_at, :], half[hi_at, :]
            paired = jnp.concatenate(
                [
                    jnp.concatenate([first[:, :det], second[:, :det]], axis=1),
                    jnp.concatenate([first[:, det:], second[:, det:]], axis=1),
                ],
                axis=0,
            )
            high, low = halves(paired)
            stacked = jnp.concatenate([high, high, low], axis=0)
            out = jnp.dot(left_f[...], stacked, preferred_element_type=f32)
            far[:, pl.ds(k * det, 2 * det)] = out
            squares = out * out
            both = squares[:det] + squares[det:]
            model = model + both[:, :det] + both[:, det:]
        factor = jnp.sqrt(patterns[p]) / jnp.sqrt(jnp.maximum(model, light_floor)) - 1.0
        wide = jnp.concatenate([factor, factor], axis=1)
        wide = jnp.concatenate([wide, wide], axis=0)
        for k in range(0, modes, 2):
            high, low = halves(far[:, pl.ds(k * det, 2 * det)] * wide)
            stacked = jnp.concatenate([high, high, low], axis=0)
            out = jnp.dot(left_b[...], stacked, preferred_element_type=f32)
            high, low = halves(out)
            for m in range(2):
                at = pl.ds((k + m) * det, det)
                for c in range(2):
                    part_h = high[c * det : (c + 1) * det, m * det : (m + 1) * det]
                    part_l = low[c * det : (c + 1) * det, m * det : (m + 1) * det]
                    deep[at, pl.ds(c * det, det)] = part_h
                    deep[at, pl.ds((2 + c) * det, det)] = part_h
                    deep[at, pl.ds((4 + c) * det, det)] = part_l
        half[...] = jnp.dot(deep[...], right_b[...], preferred_element_type=f32)
        num_re = jnp.zeros((det, det), f32)
        num_im = jnp.zeros((det, det), f32)
        for k in range(modes):
            at = pl.ds(k * det, det)
            cr, ci = half[at, :det], half[at, det:]
            pr, pi = probe[k, 0], probe[k, 1]
            grad[0, k] = grad[0, k] + patch_re * cr + patch_im * ci
            grad[1, k] = grad[1, k] + patch_re * ci - patch_im * cr
            num_re = num_re + pr * cr + pi * ci
            num_im = num_im + pr * ci - pi * cr
        zero = jnp.zeros((det, det), f32)
        for c, value in enumerate((num_re, num_im, power[...])):
            turned = pltpu.roll(value, shift, 1)
            frame[c, block, rows, :] = frame[c, block, rows, :] + jnp.where(lanes >= shift, turned, zero)
            frame[c, block + 1, rows, :] = frame[c, block + 1, rows, :] + jnp.where(lanes < shift, turned, zero)
        return total

    model_grid = lax.fori_loop(0, count, one, jnp.zeros((det, det), f32))
    measured = jnp.zeros((det, det), f32)
    for p in range(count):
        measured = measured + patterns[p]
    tiles = det // 8
    for k in range(2 * modes):
        packed[k * tiles : (k + 1) * tiles] = grad[k // modes, k % modes].reshape(tiles, 8, det)
    last = 2 * modes * tiles
    packed[last : last + tiles] = light[...].reshape(tiles, 8, det)
    packed[last + tiles] = jnp.sum(measured.reshape(tiles, 8, det), axis=0)
    packed[last + tiles + 1] = jnp.sum(model_grid.reshape(tiles, 8, det), axis=0)
    for extra in range(last + tiles + 2, packed.shape[0]):
        packed[extra] = jnp.zeros((8, det), f32)
    for c in range(3):
        for j in range(col_blocks):
            frame_out[c, :, j * det : (j + 1) * det] = frame[c, j]


def scan_positions(offsets, probe_modes, patterns, extended, block_rows, block_cols):
    modes, _, det, _ = probe_modes.shape
    f32 = jnp.float32
    ext_rows, ext_cols = extended.shape[1:]
    col_blocks = ext_cols // det
    vmem = pl.BlockSpec(memory_space=pltpu.VMEM)
    tables = [jnp.asarray(t) for t in dft_tables(det)]

    def kernel(*refs):
        scan_kernel(*refs, block_rows=block_rows, block_cols=block_cols)

    return pl.pallas_call(
        kernel,
        name="scan_positions",
        out_shape=(
            jax.ShapeDtypeStruct((packed_tiles(modes, det), 8, det), f32),
            jax.ShapeDtypeStruct((3, ext_rows, ext_cols), f32),
        ),
        in_specs=[pl.BlockSpec(memory_space=pltpu.SMEM)] + [vmem] * 7,
        out_specs=(vmem,) * 2,
        scratch_shapes=[
            pltpu.VMEM((2, col_blocks + 1, ext_rows, det), f32),
            pltpu.VMEM((3, col_blocks + 1, ext_rows, det), f32),
            pltpu.VMEM((modes * det, 6 * det), jnp.bfloat16),
            pltpu.VMEM((modes * det, 2 * det), f32),
            pltpu.VMEM((2 * det, modes * det), f32),
            pltpu.VMEM((det, det), f32),
            pltpu.VMEM((2, modes, det, det), f32),
            pltpu.VMEM((det, det), f32),
        ],
        compiler_params=pltpu.CompilerParams(vmem_limit_bytes=48 * 1024 * 1024),
    )(offsets, probe_modes, patterns, extended, *tables)


def newton_steps(gram_re, gram_im):
    mode_count = gram_re.shape[0]
    upper = jnp.concatenate([gram_re, -gram_im], axis=1)
    lower = jnp.concatenate([gram_im, gram_re], axis=1)
    embedded = jnp.concatenate([upper, lower], axis=0)
    frobenius = jnp.sqrt(jnp.sum(embedded * embedded))
    identity = jnp.eye(2 * mode_count, dtype=jnp.float32)
    current = embedded / frobenius
    inverse = identity
    for repeat in range(NS_STEPS):
        factor = 1.5 * identity - 0.5 * jnp.dot(
            inverse, current, precision=highest, preferred_element_type=jnp.float32
        )
        current = jnp.dot(current, factor, precision=highest, preferred_element_type=jnp.float32)
        inverse = jnp.dot(factor, inverse, precision=highest, preferred_element_type=jnp.float32)
    inverse = inverse / jnp.sqrt(frobenius)
    return (inverse[:mode_count, :mode_count], inverse[mode_count:, :mode_count])


def gram_parts(mode_rows):
    real_rows = mode_rows[: mode_rows.shape[0] // 2]
    imag_rows = mode_rows[mode_rows.shape[0] // 2 :]
    gram_re = jnp.dot(
        real_rows, real_rows.T, precision=highest, preferred_element_type=jnp.float32
    ) + jnp.dot(imag_rows, imag_rows.T, precision=highest, preferred_element_type=jnp.float32)
    gram_im = jnp.dot(
        real_rows, imag_rows.T, precision=highest, preferred_element_type=jnp.float32
    ) - jnp.dot(imag_rows, real_rows.T, precision=highest, preferred_element_type=jnp.float32)
    return (gram_re, gram_im)


def orthonormal_rows(mode_rows, gram_re, gram_im, power_ratio):
    real_rows = mode_rows[: mode_rows.shape[0] // 2]
    imag_rows = mode_rows[mode_rows.shape[0] // 2 :]
    mix_re, mix_im = newton_steps(gram_re, gram_im)
    ortho_re = jnp.dot(
        mix_re.T, real_rows, precision=highest, preferred_element_type=jnp.float32
    ) - jnp.dot(mix_im.T, imag_rows, precision=highest, preferred_element_type=jnp.float32)
    ortho_im = jnp.dot(
        mix_im.T, real_rows, precision=highest, preferred_element_type=jnp.float32
    ) + jnp.dot(mix_re.T, imag_rows, precision=highest, preferred_element_type=jnp.float32)
    weight = jnp.sqrt(power_ratio * jnp.diagonal(gram_re))
    return jnp.stack([ortho_re, ortho_im], axis=1) * weight[:, None, None]


fast_bits = (("scan", 1), ("scan", 2), ("scan", 4), ("tile", 1))
halvings = 3


def packed_tiles(modes, det):
    tiles = (2 * modes + 1) * (det // 8) + 2
    step = len(fast_bits) * 2**halvings
    return -(-tiles // step) * step


def mesh_bits():
    bits = list(fast_bits)
    for axis in ("scan", "tile"):
        bit = 1
        while bit < lax.axis_size(axis):
            if (axis, bit) not in bits:
                bits.append((axis, bit))
            bit *= 2
    return bits


def directions():
    return [(i, j) for i, j in ((1, 0), (-1, 0), (0, 1), (0, -1), (1, 1), (1, -1), (-1, 1), (-1, -1))]


def exchange_kernel(bits, packed, frame, out, interior, acc, landing, *rest):
    slots = rest[:8]
    send_sem, recv_sem, fold_send, fold_recv = rest[8:]
    pieces = len(fast_bits)
    piece = packed.shape[0] // pieces
    det = (frame.shape[1] - interior.shape[1]) // 2
    block_rows, block_cols = interior.shape[1:]
    here = {axis: lax.axis_index(axis) for axis in ("scan", "tile")}
    sizes = {axis: lax.axis_size(axis) for axis in ("scan", "tile")}

    def digit(axis, bit):
        return (here[axis] // bit) % 2

    def partner(axis, bit):
        return {axis: here[axis] + bit * (1 - 2 * digit(axis, bit))}

    def copy(src, dst, g, step, axis, bit):
        return pltpu.make_async_remote_copy(
            src_ref=src, dst_ref=dst, send_sem=send_sem.at[g, step], recv_sem=recv_sem.at[g, step],
            device_id=partner(axis, bit), device_id_type=pl.DeviceIdType.MESH,
        )

    plans = []
    for g in range(pieces):
        order = [fast_bits[(g + i) % pieces] for i in range(pieces)] + bits[pieces:]
        steps = []
        start, size, land = g * piece, piece, 0
        for axis, bit in order[:halvings]:
            size //= 2
            mine = digit(axis, bit)
            keep, give = start + mine * size, start + (1 - mine) * size
            steps.append(("halve", axis, bit, give, keep, size, land))
            start = keep
            land += size
        for axis, bit in order[halvings:]:
            steps.append(("both", axis, bit, start, start, size, land))
            land += size
        for axis, bit in reversed(order[:halvings]):
            low = start - digit(axis, bit) * size
            steps.append(("gather", axis, bit, start, low + (1 - digit(axis, bit)) * size, size, land))
            start = low
            land += size
            size *= 2
        plans.append(steps)
    total = len(plans[0])

    def make(g, step):
        kind, axis, bit, give, keep, size, land = plans[g][step]
        source = packed if step == 0 else acc
        src = source.at[pl.ds(give, size)]
        return copy(src, landing.at[g, pl.ds(land, size)], g, step, axis, bit)

    def settle(g, step):
        kind, axis, bit, give, keep, size, land = plans[g][step]
        source = packed if step == 0 else acc
        arrived = landing[g, pl.ds(land, size)]
        acc[pl.ds(keep, size)] = arrived if kind == "gather" else source[pl.ds(keep, size)] + arrived

    def span(shift, block):
        low = {-1: 0, 0: det, 1: det + block}[shift]
        return pl.ds(low, block if shift == 0 else det)

    def inner(shift, block):
        low = {-1: block - det, 0: 0, 1: 0}[shift]
        return pl.ds(low, block if shift == 0 else det)

    def valid(shift_rows, shift_cols):
        row, col = here["scan"] + shift_rows, here["tile"] + shift_cols
        return (row >= 0) & (row < sizes["scan"]) & (col >= 0) & (col < sizes["tile"])

    def fold(index):
        shift_rows, shift_cols = directions()[index]
        return pltpu.make_async_remote_copy(
            src_ref=frame.at[:, span(shift_rows, block_rows), span(shift_cols, block_cols)],
            dst_ref=slots[index],
            send_sem=fold_send.at[index],
            recv_sem=fold_recv.at[index],
            device_id={
                "scan": (here["scan"] + shift_rows + sizes["scan"]) % sizes["scan"],
                "tile": (here["tile"] + shift_cols + sizes["tile"]) % sizes["tile"],
            },
            device_id_type=pl.DeviceIdType.MESH,
        )

    def fold_start(indices):
        for index in indices:
            @pl.when(valid(*directions()[index]))
            def _():
                fold(index).start()

    interior[...] = frame[:, det : det + block_rows, det : det + block_cols]
    for g in range(pieces):
        make(g, 0).start()
    fold_start((0, 1))
    for step in range(total):
        for g in range(pieces):
            make(g, step).wait()
            settle(g, step)
            if step + 1 < total:
                make(g, step + 1).start()
        if step == 0:
            fold_start((2, 3))
        if step == 1:
            fold_start((4, 5, 6, 7))
    out[...] = acc[...]
    for index, (shift_rows, shift_cols) in enumerate(directions()):
        @pl.when(valid(shift_rows, shift_cols))
        def _():
            fold(index).wait_send()

        @pl.when(valid(-shift_rows, -shift_cols))
        def _():
            fold(index).wait_recv()
            rows, cols = inner(shift_rows, block_rows), inner(shift_cols, block_cols)
            interior[:, rows, cols] = interior[:, rows, cols] + slots[index][...]


def exchange(packed, frame, det, block_rows, block_cols):
    f32 = jnp.float32
    bits = mesh_bits()
    pieces = len(fast_bits)
    piece = packed.shape[0] // pieces
    steps = len(bits) + halvings
    small = piece // 2**halvings
    land = 2 * (piece - small) + (len(bits) - halvings) * small
    vmem = pl.BlockSpec(memory_space=pltpu.VMEM)
    slots = [
        pltpu.VMEM((3, det if i else block_rows, det if j else block_cols), f32) for i, j in directions()
    ]

    def kernel(*refs):
        exchange_kernel(bits, *refs)

    return pl.pallas_call(
        kernel,
        name="exchange",
        out_shape=(
            jax.ShapeDtypeStruct(packed.shape, f32),
            jax.ShapeDtypeStruct((3, block_rows, block_cols), f32),
        ),
        in_specs=[vmem, vmem],
        out_specs=(vmem, vmem),
        scratch_shapes=[
            pltpu.VMEM(packed.shape, f32),
            pltpu.VMEM((pieces, land) + packed.shape[1:], f32),
            *slots,
            pltpu.SemaphoreType.DMA((pieces, steps)),
            pltpu.SemaphoreType.DMA((pieces, steps)),
            pltpu.SemaphoreType.DMA((8,)),
            pltpu.SemaphoreType.DMA((8,)),
        ],
        compiler_params=pltpu.CompilerParams(has_side_effects=True, vmem_limit_bytes=40 * 1024 * 1024),
    )(packed, frame)


def halo_kernel(specimen, out, *rest):
    slots = rest[:8]
    send_sem, recv_sem = rest[8:]
    block_rows, block_cols = specimen.shape[1:]
    det = (out.shape[1] - block_rows) // 2
    here = {axis: lax.axis_index(axis) for axis in ("scan", "tile")}
    sizes = {axis: lax.axis_size(axis) for axis in ("scan", "tile")}

    def edge(shift, block):
        low = {-1: 0, 0: 0, 1: block - det}[shift]
        return pl.ds(low, block if shift == 0 else det)

    def outer(shift, block):
        low = {-1: det + block, 0: det, 1: 0}[shift]
        return pl.ds(low, block if shift == 0 else det)

    def valid(shift_rows, shift_cols):
        row, col = here["scan"] + shift_rows, here["tile"] + shift_cols
        return (row >= 0) & (row < sizes["scan"]) & (col >= 0) & (col < sizes["tile"])

    def send(index):
        shift_rows, shift_cols = directions()[index]
        return pltpu.make_async_remote_copy(
            src_ref=specimen.at[:, edge(shift_rows, block_rows), edge(shift_cols, block_cols)],
            dst_ref=slots[index],
            send_sem=send_sem.at[index],
            recv_sem=recv_sem.at[index],
            device_id={
                "scan": (here["scan"] + shift_rows + sizes["scan"]) % sizes["scan"],
                "tile": (here["tile"] + shift_cols + sizes["tile"]) % sizes["tile"],
            },
            device_id_type=pl.DeviceIdType.MESH,
        )

    for index, shifts in enumerate(directions()):
        @pl.when(valid(*shifts))
        def _():
            send(index).start()
    out[...] = jnp.zeros_like(out)
    out[:, det : det + block_rows, det : det + block_cols] = specimen[...]
    for index, (shift_rows, shift_cols) in enumerate(directions()):
        @pl.when(valid(shift_rows, shift_cols))
        def _():
            send(index).wait_send()

        @pl.when(valid(-shift_rows, -shift_cols))
        def _():
            send(index).wait_recv()
            out[:, outer(shift_rows, block_rows), outer(shift_cols, block_cols)] = slots[index][...]


def with_halo(specimen, det):
    channels, block_rows, block_cols = specimen.shape
    vmem = pl.BlockSpec(memory_space=pltpu.VMEM)
    slots = [
        pltpu.VMEM((channels, det if i else block_rows, det if j else block_cols), jnp.float32)
        for i, j in directions()
    ]
    return pl.pallas_call(
        halo_kernel,
        name="halo",
        out_shape=jax.ShapeDtypeStruct((channels, block_rows + 2 * det, block_cols + 2 * det), jnp.float32),
        in_specs=[vmem],
        out_specs=vmem,
        scratch_shapes=[*slots, pltpu.SemaphoreType.DMA((8,)), pltpu.SemaphoreType.DMA((8,))],
        compiler_params=pltpu.CompilerParams(has_side_effects=True, vmem_limit_bytes=16 * 1024 * 1024),
    )(specimen)


def body(probe_modes, patterns, specimen, offsets):
    detector = probe_modes.shape[-1]
    mode_count = probe_modes.shape[0]
    block_rows = specimen.shape[1]
    block_cols = specimen.shape[2]
    extended = with_halo(specimen, detector)
    packed, frame_sum = scan_positions(
        offsets, probe_modes, patterns, extended, block_rows, block_cols
    )
    summed, interior = exchange(packed, frame_sum, detector, block_rows, block_cols)
    pixels = detector * detector
    tiles = detector // 8
    last = 2 * mode_count * tiles
    grad_total = summed[:last].reshape(2 * mode_count, pixels)
    light_total = summed[last : last + tiles].reshape(1, pixels)
    measured_all = jnp.sum(summed[last + tiles])
    model_all = jnp.sum(summed[last + tiles + 1])
    power_ratio = measured_all / (model_all + total_eps)
    new_specimen = specimen + interior[0:2] / (interior[2] + object_reg)[None]
    probe_rows = jnp.swapaxes(probe_modes, 0, 1).reshape(2 * mode_count, pixels)
    updated = probe_rows + grad_total / (light_total + probe_reg)
    gram_re, gram_im = gram_parts(updated)
    new_probe = orthonormal_rows(updated, gram_re, gram_im, power_ratio).reshape(probe_modes.shape)
    return (new_probe, new_specimen)


def solution(mesh):
    return jax.shard_map(
        body,
        mesh=mesh,
        in_specs=(
            P(),
            P(("scan", "tile"), None, None),
            P(None, "scan", "tile"),
            P(("scan", "tile"), None),
        ),
        out_specs=(P(), P(None, "scan", "tile")),
        check_vma=False,
    )
```
